32 devices in a mesh: sample: 8 (over y, x, core), line: 4 (over z).
Axes of the slice: x: 2, y: 2, z: 4, core: 2. Of those that a mesh axis runs over, the one named last changes fastest.
Arguments:
- wind_dev: bfloat16 [4096, 10000], P('sample', 'line'), may hold values from -6 to 6
- ptdf: bfloat16 [4096, 10000], P('line'), may hold values from -0.0625 to 0.0625
- region_weights: bfloat16 [31, 10000], replicated, may hold values from -0.0625 to 0.0625
- incidence: int32 [12706, 2], replicated, may hold values from 0 to 9999
- monitored: int32 [4096], P('line'), may hold values from 0 to 12705
- ratings: float32 [12706], replicated, may hold values from 1 to 3
- base_flow: float32 [4096], P('line'), may hold values from -6 to 6
- line_cost: float32 [4096], P('line'), may hold values from 0.2 to 20
- policy: float32 [32, 4096], P(None, 'line'), may hold values from -0.6 to 0.6
Outputs:
- new_policy: float32 [32, 4096], P(None, 'line')
- new_flows: float32 [4096, 4096], P('sample', 'line')
- decrement: float32 [], replicated
- grad_norm: float32 [], replicated
The draws below stay inside these ranges and needn't reach their ends.
All inputs are finite; a program needn't handle non-finite values.
Results may differ from the reference program's by a relative error of at most 0.0003.
Values may be sent and summed in bfloat16 or wider, within the bound.
A program may use at most 128 MiB of HBM per device.

```python
import math
import jax
import jax.numpy as jnp
from jax import lax

NUM_BUSES = 10000
MONITORED = 4096
GRID_LINES = 12706
REGIONS = 31
FEATURES = 32
SCENARIOS = 4096


def draw_line_cost(key, part):
    position = jnp.arange(MONITORED, dtype=jnp.float32) / MONITORED
    low_end = 0.3
    high_end = 3.0
    rise_rate = 1.1
    uniform_draw = jax.random.uniform(key, (MONITORED,), jnp.float32)
    spread_term = jnp.exp(jnp.log(low_end) + uniform_draw * (jnp.log(high_end) - jnp.log(low_end)))
    return spread_term * jnp.exp(rise_rate * position)


def with_ends(drawn, rng, low, high):
    longest = drawn.shape.index(max(drawn.shape))
    spots = []
    for shift in (0, 1):
        where = [jax.random.randint(jax.random.fold_in(rng, axis), (), 0, length) for axis, length in enumerate(drawn.shape)]
        where[longest] = (where[longest] + shift) % drawn.shape[longest]
        spots.append(tuple(where))
    return drawn.at[spots[0]].set(low).at[spots[1]].set(high)


def steps_of(own_key, extent, cuts, low, largest):
    loudness, own = 1.0, jax.random.fold_in(own_key, 6)
    for dim, parts in cuts:
        steps = jnp.exp(jax.random.uniform(jax.random.fold_in(own, dim), (parts,), jnp.float32, low / len(cuts), largest / len(cuts)))
        loudness = loudness * jnp.repeat(steps, extent[dim] // parts).reshape([-1 if axis == dim else 1 for axis in range(len(extent))])
    return loudness


def noise(stream_key, dims, scale, reach, shards=(), held_as=jnp.bfloat16):
    result = jax.random.normal(stream_key, dims, jnp.float32) * scale
    if len(shards) > 0:
        result = steps_of(stream_key, dims, shards, -0.22, 0.18) * result
    return jnp.clip(result, min=-reach, max=reach).astype(held_as)


def setup_inputs(seed: int = 0) -> dict:
    key_of = jax.random.split(jax.random.key(seed), 10)
    return {
        "wind_dev": noise(key_of[0], (SCENARIOS, NUM_BUSES), 1.0, 6.0, ((0, 8), (1, 4))),
        "ptdf": noise(key_of[1], (MONITORED, NUM_BUSES), NUM_BUSES ** -0.5, 0.0625, ((0, 4),)),
        "region_weights": noise(key_of[2], (REGIONS, NUM_BUSES), NUM_BUSES ** -0.5, 0.0625),
        "incidence": with_ends(jax.random.randint(key_of[3], (GRID_LINES, 2), 0, NUM_BUSES), jax.random.fold_in(key_of[3], 1), 0, NUM_BUSES - 1).astype(jnp.int32),
        "monitored": with_ends(jax.random.randint(key_of[4], (MONITORED,), 0, GRID_LINES), jax.random.fold_in(key_of[4], 1), 0, GRID_LINES - 1).astype(jnp.int32),
        "ratings": jnp.clip(jnp.exp(jax.random.uniform(key_of[5], (GRID_LINES,), jnp.float32, math.log(1.0), math.log(3.0))), 1.0, 3.0),
        "base_flow": noise(key_of[6], (MONITORED,), 1.0, 6.0, ((0, 4),), jnp.float32),
        "line_cost": draw_line_cost(jax.random.fold_in(key_of[9], 71), 0),
        "policy": jnp.clip(jax.random.uniform(key_of[8], (FEATURES, MONITORED), jnp.float32, -0.6, 0.6) * steps_of(key_of[8], (FEATURES, MONITORED), ((1, 4),), -0.4, 0.0), -0.6, 0.6),
    }


ridge_weight = 1.0
barrier_weight = 0.1
smoothing = 0.5

def penalty_terms(factors, ends_diff, slope_term, curve_term, weight):
    highest = lax.Precision.HIGHEST
    regions = factors.shape[1]
    lines_here = slope_term.shape[1]
    outer_prod = (factors[:, :, None] * factors[:, None, :]).reshape(factors.shape[0], regions * regions)
    block_rr = lax.dot_general(outer_prod, curve_term, (((0,), (0,)), ((), ())), precision=highest)
    weighted = curve_term * ends_diff
    cross_re = lax.dot_general(factors, weighted, (((0,), (0,)), ((), ())), precision=highest)
    corner = lax.optimization_barrier(jnp.sum(weighted * ends_diff, axis=0))
    upper_rows = jnp.concatenate([block_rr.reshape(regions, regions, lines_here), cross_re[:, None, :]], axis=1)
    bottom = jnp.concatenate([cross_re[None, :, :], corner[None, None, :]], axis=1)
    hessian = jnp.concatenate([upper_rows, bottom], axis=0) * weight
    grad_rr = lax.dot_general(factors, slope_term, (((0,), (0,)), ((), ())), precision=highest)
    gradient = jnp.concatenate([grad_rr, lax.optimization_barrier(jnp.sum(slope_term * ends_diff, axis=0))[None, :]], axis=0) * weight
    return (hessian.reshape((regions + 1) * (regions + 1), lines_here), gradient)

def factor_solve(hessian, gradient):
    features = gradient.shape[0]
    positions = jnp.arange(features, dtype=jnp.int32)

    def chol_column(column, lower_tri):
        target = lax.dynamic_index_in_dim(hessian, column, 1, keepdims=False)
        row_here = lax.dynamic_index_in_dim(lower_tri, column, 0, keepdims=False)
        running = target - lax.optimization_barrier(jnp.sum(lower_tri * row_here[None, :, :], axis=1))
        pivot_val = jnp.sqrt(lax.dynamic_index_in_dim(running, column, 0, keepdims=False))
        new_col = jnp.where((positions >= column)[:, None], running / pivot_val[None, :], jnp.zeros_like(running))
        select = (positions == column).astype(hessian.dtype)
        return lower_tri + new_col[:, None, :] * select[None, :, None]
    lower_tri = lax.fori_loop(0, features, chol_column, jnp.zeros_like(hessian))

    def forward_row(row_index, forward):
        row_here = lax.dynamic_index_in_dim(lower_tri, row_index, 0, keepdims=False)
        running = lax.dynamic_index_in_dim(gradient, row_index, 0, keepdims=False) - lax.optimization_barrier(jnp.sum(row_here * forward, axis=0))
        value = running / lax.dynamic_index_in_dim(row_here, row_index, 0, keepdims=False)
        select = (positions == row_index).astype(gradient.dtype)
        return forward + select[:, None] * value[None, :]
    forward = lax.fori_loop(0, features, forward_row, jnp.zeros_like(gradient))

    def backward_row(turn, backward):
        row_index = features - 1 - turn
        col_here = lax.dynamic_index_in_dim(lower_tri, row_index, 1, keepdims=False)
        running = lax.dynamic_index_in_dim(forward, row_index, 0, keepdims=False) - lax.optimization_barrier(jnp.sum(col_here * backward, axis=0))
        value = running / lax.dynamic_index_in_dim(col_here, row_index, 0, keepdims=False)
        select = (positions == row_index).astype(gradient.dtype)
        return backward + select[:, None] * value[None, :]
    backward = lax.fori_loop(0, features, backward_row, jnp.zeros_like(gradient))
    return (forward, -backward)

def owner_step(hessian_flat, gradient, policy_part):
    features = gradient.shape[0]
    lines_here = gradient.shape[1]
    hessian = hessian_flat.reshape(features, features, lines_here)
    margin_sq = 1.0 - policy_part * policy_part
    diag_terms = ridge_weight + barrier_weight * 2.0 * (1.0 + policy_part * policy_part) / (margin_sq * margin_sq)
    hessian = hessian + jnp.eye(features, dtype=hessian.dtype)[:, :, None] * diag_terms[:, None, :]
    gradient = gradient + ridge_weight * policy_part + barrier_weight * 2.0 * policy_part / margin_sq
    forward, newton_step = factor_solve(hessian, gradient)
    return (gradient, forward, newton_step)

def reference(wind_dev, ptdf, region_weights, incidence, monitored, ratings, base_flow, line_cost, policy):
    highest = lax.Precision.HIGHEST
    regions = region_weights.shape[0]
    endpoints = jnp.take(incidence, monitored, axis=0)
    from_bus = endpoints[:, 0]
    to_bus = endpoints[:, 1]
    rating = jnp.take(ratings, monitored)
    total_scen = wind_dev.shape[0]
    grid_flow = jnp.dot(wind_dev, ptdf.T, preferred_element_type=jnp.float32)
    factors = jnp.dot(wind_dev, region_weights.T, preferred_element_type=jnp.float32)
    ends_diff = jnp.take(wind_dev, to_bus, axis=1).astype(jnp.float32) - jnp.take(wind_dev, from_bus, axis=1).astype(jnp.float32)
    line_flow = grid_flow + base_flow[None, :] + jnp.dot(factors, policy[:regions], precision=highest) + policy[regions][None, :] * ends_diff
    prob_up = jax.nn.sigmoid((line_flow - rating[None, :]) / smoothing)
    prob_down = jax.nn.sigmoid((-line_flow - rating[None, :]) / smoothing)
    slope_term = prob_up - prob_down
    curve_term = (prob_up * (1.0 - prob_up) + prob_down * (1.0 - prob_down)) / smoothing
    weight = line_cost / total_scen
    hessian_sum, gradient_sum = penalty_terms(factors, ends_diff, slope_term, curve_term, weight)
    gradient, forward, newton_step = owner_step(hessian_sum, gradient_sum, policy)
    decrement_sq = jnp.sum(forward * forward)
    norm_sq = jnp.sum(gradient * gradient)
    features = policy.shape[0]
    step_length = 1.0 / (1.0 + jnp.sqrt(decrement_sq / (barrier_weight * features * MONITORED)))
    new_policy = policy + step_length * newton_step
    shift_flow = jnp.dot(factors, newton_step[:regions], precision=highest) + newton_step[regions][None, :] * ends_diff
    new_flows = line_flow + step_length * shift_flow
    return (new_policy, new_flows, jnp.sqrt(decrement_sq), jnp.sqrt(norm_sq))
```

```python
import jax
import jax.numpy as jnp
from jax import lax
from jax.experimental import pallas as pl
from jax.experimental.pallas import tpu as pltpu
from jax.sharding import PartitionSpec as P

ridge_weight = 1.0
barrier_weight = 0.1
smoothing = 0.5


HIGH = lax.Precision.HIGH


def hop(piece, shift):
    ring = lax.axis_size("line")
    return lax.ppermute(piece, "line", [(i, (i + shift) % ring) for i in range(ring)])


def ring_pieces(wind_dev):
    ring = lax.axis_size("line")
    me = lax.axis_index("line")
    pieces = [(wind_dev, me)]
    up = down = wind_dev
    for step in range(1, (ring - 1) // 2 + 1):
        up, down = hop(up, 1), hop(down, -1)
        pieces.append((up, lax.rem(me - step + ring, ring)))
        pieces.append((down, lax.rem(me + step, ring)))
    if ring % 2 == 0:
        half = wind_dev.shape[0] // 2
        far = jnp.concatenate([hop(up[:half], 1), hop(down[half:], -1)], axis=0)
        pieces.append((far, lax.rem(me + ring // 2, ring)))
    return pieces


def solve_lines(regions, packed_ref, weight_ref, policy_ref, out_ref, cols_ref):
    features = regions + 1
    weight = weight_ref[...]
    policy = policy_ref[...]
    margin_sq = 1.0 - policy * policy
    diag_terms = ridge_weight + barrier_weight * 2.0 * (1.0 + policy * policy) / (
        margin_sq * margin_sq
    )
    cols_ref[...] = jnp.zeros_like(cols_ref)
    bands = (regions + 1) // 2
    for band in range(bands):
        rows = packed_ref[band * features : (band + 1) * features, :] * weight
        if band == 0:
            rows = rows + diag_terms
        for i in range(regions):
            j = (i + band) % regions
            cols_ref[min(i, j), max(i, j) : max(i, j) + 1, :] = rows[i : i + 1]
    cross = packed_ref[bands * features : (bands + 1) * features, :] * weight
    for i in range(regions):
        cols_ref[i, regions : regions + 1, :] = cross[i : i + 1]
    cols_ref[regions, regions : regions + 1, :] = cross[regions:] + diag_terms[regions:]
    gradient = packed_ref[(bands + 1) * features : (bands + 2) * features, :] * weight
    gradient = gradient + ridge_weight * policy + barrier_weight * 2.0 * policy / margin_sq
    grad_sq = jnp.sum(gradient * gradient, axis=0, keepdims=True)

    positions = lax.broadcasted_iota(jnp.int32, gradient.shape, 0)
    inverses, forward = [], []
    running = gradient
    forward_sq = jnp.zeros_like(weight)
    for k in range(features):
        column = cols_ref[k]
        inverse = 1.0 / jnp.sqrt(column[k : k + 1])
        column = jnp.where(positions >= k, column * inverse, 0.0)
        cols_ref[k] = column
        value = running[k : k + 1] * inverse
        running = running - column * value
        forward_sq = forward_sq + value * value
        inverses.append(inverse)
        forward.append(value)
        for j in range(k + 1, features):
            base = j // 8 * 8
            cols_ref[j, base:, :] = cols_ref[j, base:, :] - column[base:] * column[j : j + 1]
    solved = jnp.zeros_like(gradient)
    for k in reversed(range(features)):
        value = (
            forward[k] - jnp.sum(cols_ref[k] * solved, axis=0, keepdims=True)
        ) * inverses[k]
        solved = jnp.where(positions == k, value, solved)
    out_ref[...] = jnp.zeros_like(out_ref)
    out_ref[:features, :] = -solved
    out_ref[features : features + 1, :] = forward_sq
    out_ref[features + 1 : features + 2, :] = grad_sq


def shards(
    wind_dev, ptdf, region_weights, incidence, monitored, ratings, base_flow, line_cost, policy
):
    regions = region_weights.shape[0]
    features = regions + 1
    scen_here, width = wind_dev.shape
    lines_here = ptdf.shape[0]
    ring = lax.axis_size("line")
    samples = lax.axis_size("sample")

    pieces = ring_pieces(wind_dev)

    endpoints = jnp.take(incidence, monitored, axis=0)
    from_bus = endpoints[:, 0]
    to_bus = endpoints[:, 1]
    rating = jnp.take(ratings, monitored)
    ptdf_pieces = ptdf.reshape(lines_here, ring, width).transpose(1, 0, 2)
    weight_pieces = (
        jnp.pad(region_weights, ((0, 1), (0, 0))).reshape(features, ring, width).transpose(1, 0, 2)
    )

    grid_flow = ends_diff = factors = 0.0
    buses = lax.broadcasted_iota(jnp.int32, (lines_here, width), 1)
    for piece, owner in pieces:
        here = buses + owner * width
        pick = (here == to_bus[:, None]).astype(jnp.bfloat16) - (
            here == from_bus[:, None]
        ).astype(jnp.bfloat16)
        ptdf_piece = lax.dynamic_index_in_dim(ptdf_pieces, owner, 0, keepdims=False)
        weight_piece = lax.dynamic_index_in_dim(weight_pieces, owner, 0, keepdims=False)
        pick, ptdf_piece = lax.optimization_barrier((pick, ptdf_piece))
        over_buses = (((1,), (1,)), ((), ()))
        grid_flow = grid_flow + lax.dot_general(
            piece, ptdf_piece, over_buses, preferred_element_type=jnp.float32
        )
        ends_diff = ends_diff + lax.dot_general(
            piece, pick, over_buses, preferred_element_type=jnp.float32
        )
        factors = factors + lax.dot_general(
            weight_piece, piece, over_buses, preferred_element_type=jnp.float32
        )

    over_first = (((0,), (0,)), ((), ()))
    over_scen = (((1,), (0,)), ((), ()))
    line_flow = (
        grid_flow
        + base_flow[None, :]
        + lax.dot_general(factors, policy, over_first, precision=HIGH)
        + policy[regions][None, :] * ends_diff
    )
    prob_up = jax.nn.sigmoid((line_flow - rating[None, :]) / smoothing)
    prob_down = jax.nn.sigmoid((-line_flow - rating[None, :]) / smoothing)
    slope_term = prob_up - prob_down
    curve_term = (prob_up * (1.0 - prob_up) + prob_down * (1.0 - prob_down)) / smoothing
    weighted = curve_term * ends_diff

    doubled = jnp.concatenate([factors[:regions], factors[:regions], factors[regions:]], axis=0)
    bands = (regions + 1) // 2
    pairs = jnp.concatenate([doubled[d : d + features] * factors for d in range(bands)], axis=0)
    packed = jnp.concatenate(
        [
            lax.dot_general(pairs, curve_term, over_scen, precision=HIGH),
            lax.dot_general(factors, weighted, over_scen, precision=HIGH)[:regions],
            jnp.sum(weighted * ends_diff, axis=0)[None, :],
            lax.dot_general(factors, slope_term, over_scen, precision=HIGH)[:regions],
            jnp.sum(slope_term * ends_diff, axis=0)[None, :],
        ],
        axis=0,
    )
    packed = lax.psum_scatter(packed, "sample", scatter_dimension=1, tiled=True)
    share = packed.shape[1]
    start = lax.axis_index("sample") * share
    weight_share = lax.dynamic_slice_in_dim(line_cost, start, share)[None, :] / (
        scen_here * samples
    )
    policy_share = lax.dynamic_slice_in_dim(policy, start, share, 1)
    solved = pl.pallas_call(
        lambda *refs: solve_lines(regions, *refs),
        out_shape=jax.ShapeDtypeStruct((features + 8, share), jnp.float32),
        scratch_shapes=[pltpu.VMEM((features, features, share), jnp.float32)],
        name="solve_lines",
    )(packed, weight_share, policy_share)
    gathered = lax.all_gather(solved, "sample", axis=1, tiled=True)
    full_step = gathered[:features]
    sums = jnp.sum(gathered[features : features + 2], axis=1)
    decrement_sq, norm_sq = jnp.sum(lax.all_gather(sums, "line"), axis=0)

    total_lines = lines_here * ring
    step_length = 1.0 / (1.0 + jnp.sqrt(decrement_sq / (barrier_weight * features * total_lines)))
    new_policy = policy + step_length * full_step
    shift_flow = (
        lax.dot_general(factors, full_step, over_first, precision=HIGH)
        + full_step[regions][None, :] * ends_diff
    )
    new_flows = line_flow + step_length * shift_flow
    return (new_policy, new_flows, jnp.sqrt(decrement_sq), jnp.sqrt(norm_sq))


def solution(mesh):
    placed = (
        P("sample", "line"),
        P("line", None),
        P(),
        P(),
        P("line"),
        P(),
        P("line"),
        P("line"),
        P(None, "line"),
    )
    return jax.shard_map(
        shards,
        mesh=mesh,
        in_specs=placed,
        out_specs=(P(None, "line"), P("sample", "line"), P(), P()),
        check_vma=False,
    )
```

```python
import jax
import jax.numpy as jnp
from jax import lax
from jax.experimental import pallas as pl
from jax.experimental.pallas import tpu as pltpu
from jax.sharding import PartitionSpec as P

ridge_weight = 1.0
barrier_weight = 0.1
smoothing = 0.5


HIGH = lax.Precision.HIGH


def hop(piece, shift):
    ring = lax.axis_size("line")
    return lax.ppermute(piece, "line", [(i, (i + shift) % ring) for i in range(ring)])


def ring_pieces(wind_dev):
    ring = lax.axis_size("line")
    me = lax.axis_index("line")
    pieces = [(wind_dev, me)]
    up = down = wind_dev
    for step in range(1, (ring - 1) // 2 + 1):
        up, down = hop(up, 1), hop(down, -1)
        pieces.append((up, lax.rem(me - step + ring, ring)))
        pieces.append((down, lax.rem(me + step, ring)))
    if ring % 2 == 0:
        half = wind_dev.shape[0] // 2
        far = jnp.concatenate([hop(up[:half], 1), hop(down[half:], -1)], axis=0)
        pieces.append((far, lax.rem(me + ring // 2, ring)))
    return pieces


def solve_lines(regions, packed_ref, weight_ref, policy_ref, out_ref, cols_ref):
    features = regions + 1
    weight = weight_ref[...]
    policy = policy_ref[...]
    margin_sq = 1.0 - policy * policy
    diag_terms = ridge_weight + barrier_weight * 2.0 * (1.0 + policy * policy) / (
        margin_sq * margin_sq
    )
    cols_ref[...] = jnp.zeros_like(cols_ref)
    bands = (regions + 1) // 2
    for band in range(bands):
        rows = packed_ref[band * features : (band + 1) * features, :] * weight
        if band == 0:
            rows = rows + diag_terms
        for i in range(regions):
            j = (i + band) % regions
            cols_ref[min(i, j), max(i, j) : max(i, j) + 1, :] = rows[i : i + 1]
    cross = packed_ref[bands * features : (bands + 1) * features, :] * weight
    for i in range(regions):
        cols_ref[i, regions : regions + 1, :] = cross[i : i + 1]
    cols_ref[regions, regions : regions + 1, :] = cross[regions:] + diag_terms[regions:]
    gradient = packed_ref[(bands + 1) * features : (bands + 2) * features, :] * weight
    gradient = gradient + ridge_weight * policy + barrier_weight * 2.0 * policy / margin_sq
    grad_sq = jnp.sum(gradient * gradient, axis=0, keepdims=True)

    positions = lax.broadcasted_iota(jnp.int32, gradient.shape, 0)
    inverses, forward = [], []
    running = gradient
    forward_sq = jnp.zeros_like(weight)
    for k in range(features):
        column = cols_ref[k]
        inverse = 1.0 / jnp.sqrt(column[k : k + 1])
        column = jnp.where(positions >= k, column * inverse, 0.0)
        cols_ref[k] = column
        value = running[k : k + 1] * inverse
        running = running - column * value
        forward_sq = forward_sq + value * value
        inverses.append(inverse)
        forward.append(value)
        for j in range(k + 1, features):
            base = j // 8 * 8
            cols_ref[j, base:, :] = cols_ref[j, base:, :] - column[base:] * column[j : j + 1]
    solved = jnp.zeros_like(gradient)
    for k in reversed(range(features)):
        value = (
            forward[k] - jnp.sum(cols_ref[k] * solved, axis=0, keepdims=True)
        ) * inverses[k]
        solved = jnp.where(positions == k, value, solved)
    out_ref[...] = jnp.zeros_like(out_ref)
    out_ref[:features, :] = -solved
    out_ref[features : features + 1, :] = forward_sq
    out_ref[features + 1 : features + 2, :] = grad_sq


def greet(partners):
    barrier = pltpu.get_barrier_semaphore()
    for partner in partners:
        pl.semaphore_signal(
            barrier, inc=1, device_id=partner, device_id_type=pl.DeviceIdType.MESH
        )
    pl.semaphore_wait(barrier, len(partners))


def sum_shares(samples, parts_ref, out_ref, near_ref, sums_ref, far_ref, sends, recvs):
    me = lax.axis_index("sample")
    pairs = samples // 2
    mine, side = me // 2, lax.rem(me, 2)
    others = [lax.rem(mine + i, pairs) for i in range(1, pairs)]
    partner = 2 * mine + (1 - side)
    greet([{"sample": partner}] + [{"sample": 2 * pair + side} for pair in others])
    near = []
    for slot, pair in enumerate(others + [mine]):
        near.append(
            pltpu.make_async_remote_copy(
                src_ref=parts_ref.at[2 * pair + (1 - side)],
                dst_ref=near_ref.at[slot],
                send_sem=sends.at[slot],
                recv_sem=recvs.at[slot],
                device_id={"sample": partner},
                device_id_type=pl.DeviceIdType.MESH,
            )
        )
        near[-1].start()
    for slot, pair in enumerate(others + [mine]):
        near[slot].wait_recv()
        sums_ref[slot] = parts_ref[2 * pair + side] + near_ref[slot]
    far = []
    for slot, pair in enumerate(others):
        far.append(
            pltpu.make_async_remote_copy(
                src_ref=sums_ref.at[slot],
                dst_ref=far_ref.at[slot],
                send_sem=sends.at[pairs + slot],
                recv_sem=recvs.at[pairs + slot],
                device_id={"sample": 2 * pair + side},
                device_id_type=pl.DeviceIdType.MESH,
            )
        )
        far[-1].start()
    out_ref[...] = sums_ref[pairs - 1]
    for slot in range(pairs - 1):
        far[slot].wait_recv()
        out_ref[...] += far_ref[slot]
    for copy in near + far:
        copy.wait_send()


def scatter_sum(packed):
    samples = lax.axis_size("sample")
    rows, lines = packed.shape
    share = lines // samples
    pairs = samples // 2
    parts = packed.reshape(rows, samples, share).transpose(1, 0, 2)
    return pl.pallas_call(
        lambda *refs: sum_shares(samples, *refs),
        out_shape=jax.ShapeDtypeStruct((rows, share), packed.dtype),
        in_specs=[pl.BlockSpec(memory_space=pltpu.VMEM)],
        out_specs=pl.BlockSpec(memory_space=pltpu.VMEM),
        scratch_shapes=[
            pltpu.VMEM((pairs, rows, share), packed.dtype),
            pltpu.VMEM((pairs, rows, share), packed.dtype),
            pltpu.VMEM((pairs - 1, rows, share), packed.dtype),
            pltpu.SemaphoreType.DMA((2 * pairs - 1,)),
            pltpu.SemaphoreType.DMA((2 * pairs - 1,)),
        ],
        compiler_params=pltpu.CompilerParams(collective_id=0, has_side_effects=True),
        name="scatter_sum",
    )(parts)


def share_steps(samples, ring, features, solved_ref, all_ref, sums_ref, got_ref, mine_ref, far_ref, sends, recvs):
    me, place = lax.axis_index("sample"), lax.axis_index("line")
    peers = [lax.rem(me + i, samples) for i in range(1, samples)]
    lines = [lax.rem(place + i, ring) for i in range(1, ring)]
    greet([{"sample": peer} for peer in peers] + [{"line": line} for line in lines])
    copies = []
    for slot, peer in enumerate(peers):
        copies.append(
            pltpu.make_async_remote_copy(
                src_ref=solved_ref,
                dst_ref=got_ref.at[slot],
                send_sem=sends.at[slot],
                recv_sem=recvs.at[slot],
                device_id={"sample": peer},
                device_id_type=pl.DeviceIdType.MESH,
            )
        )
        copies[-1].start()
    total = solved_ref[features:, :]
    for slot in range(samples - 1):
        copies[slot].wait_recv()
        total = total + got_ref[slot, features:, :]
    mine_ref[...] = total
    all_ref[me] = solved_ref[:features, :]
    for slot in range(samples - 1):
        source = lax.rem(me + samples - 1 - slot, samples)
        all_ref[source] = got_ref[slot, :features, :]
    far = []
    for slot, line in enumerate(lines):
        far.append(
            pltpu.make_async_remote_copy(
                src_ref=mine_ref,
                dst_ref=far_ref.at[slot],
                send_sem=sends.at[samples - 1 + slot],
                recv_sem=recvs.at[samples - 1 + slot],
                device_id={"line": line},
                device_id_type=pl.DeviceIdType.MESH,
            )
        )
        far[-1].start()
    total = mine_ref[...]
    for slot in range(ring - 1):
        far[slot].wait_recv()
        total = total + far_ref[slot]
    sums_ref[...] = total
    for copy in copies + far:
        copy.wait_send()


def gather_steps(solved, features):
    samples, ring = lax.axis_size("sample"), lax.axis_size("line")
    rows, share = solved.shape
    vmem = pl.BlockSpec(memory_space=pltpu.VMEM)
    copies = samples + ring - 2
    return pl.pallas_call(
        lambda *refs: share_steps(samples, ring, features, *refs),
        out_shape=(
            jax.ShapeDtypeStruct((samples, features, share), solved.dtype),
            jax.ShapeDtypeStruct((rows - features, share), solved.dtype),
        ),
        in_specs=[vmem],
        out_specs=(vmem, vmem),
        scratch_shapes=[
            pltpu.VMEM((samples - 1, rows, share), solved.dtype),
            pltpu.VMEM((rows - features, share), solved.dtype),
            pltpu.VMEM((ring - 1, rows - features, share), solved.dtype),
            pltpu.SemaphoreType.DMA((copies,)),
            pltpu.SemaphoreType.DMA((copies,)),
        ],
        compiler_params=pltpu.CompilerParams(collective_id=1, has_side_effects=True),
        name="gather_steps",
    )(solved)


def shards(
    wind_dev, ptdf, region_weights, incidence, monitored, ratings, base_flow, line_cost, policy
):
    regions = region_weights.shape[0]
    features = regions + 1
    scen_here, width = wind_dev.shape
    lines_here = ptdf.shape[0]
    ring = lax.axis_size("line")
    samples = lax.axis_size("sample")

    pieces = ring_pieces(wind_dev)

    endpoints = jnp.take(incidence, monitored, axis=0)
    from_bus = endpoints[:, 0]
    to_bus = endpoints[:, 1]
    rating = jnp.take(ratings, monitored)
    ptdf_pieces = ptdf.reshape(lines_here, ring, width).transpose(1, 0, 2)
    weight_pieces = (
        jnp.pad(region_weights, ((0, 1), (0, 0))).reshape(features, ring, width).transpose(1, 0, 2)
    )

    grid_flow = ends_diff = factors = 0.0
    buses = lax.broadcasted_iota(jnp.int32, (lines_here, width), 1)
    for piece, owner in pieces:
        here = buses + owner * width
        pick = (here == to_bus[:, None]).astype(jnp.bfloat16) - (
            here == from_bus[:, None]
        ).astype(jnp.bfloat16)
        ptdf_piece = lax.dynamic_index_in_dim(ptdf_pieces, owner, 0, keepdims=False)
        weight_piece = lax.dynamic_index_in_dim(weight_pieces, owner, 0, keepdims=False)
        pick, ptdf_piece = lax.optimization_barrier((pick, ptdf_piece))
        over_buses = (((1,), (1,)), ((), ()))
        grid_flow = grid_flow + lax.dot_general(
            piece, ptdf_piece, over_buses, preferred_element_type=jnp.float32
        )
        ends_diff = ends_diff + lax.dot_general(
            piece, pick, over_buses, preferred_element_type=jnp.float32
        )
        factors = factors + lax.dot_general(
            weight_piece, piece, over_buses, preferred_element_type=jnp.float32
        )

    over_first = (((0,), (0,)), ((), ()))
    over_scen = (((1,), (0,)), ((), ()))
    line_flow = (
        grid_flow
        + base_flow[None, :]
        + lax.dot_general(factors, policy, over_first, precision=HIGH)
        + policy[regions][None, :] * ends_diff
    )
    prob_up = jax.nn.sigmoid((line_flow - rating[None, :]) / smoothing)
    prob_down = jax.nn.sigmoid((-line_flow - rating[None, :]) / smoothing)
    slope_term = prob_up - prob_down
    curve_term = (prob_up * (1.0 - prob_up) + prob_down * (1.0 - prob_down)) / smoothing
    weighted = curve_term * ends_diff

    doubled = jnp.concatenate([factors[:regions], factors[:regions], factors[regions:]], axis=0)
    bands = (regions + 1) // 2
    pairs = jnp.concatenate([doubled[d : d + features] * factors for d in range(bands)], axis=0)
    packed = jnp.concatenate(
        [
            lax.dot_general(pairs, curve_term, over_scen, precision=HIGH),
            lax.dot_general(factors, weighted, over_scen, precision=HIGH)[:regions],
            jnp.sum(weighted * ends_diff, axis=0)[None, :],
            lax.dot_general(factors, slope_term, over_scen, precision=HIGH)[:regions],
            jnp.sum(slope_term * ends_diff, axis=0)[None, :],
        ],
        axis=0,
    )
    packed = scatter_sum(packed)
    share = packed.shape[1]
    start = lax.axis_index("sample") * share
    weight_share = lax.dynamic_slice_in_dim(line_cost, start, share)[None, :] / (
        scen_here * samples
    )
    policy_share = lax.dynamic_slice_in_dim(policy, start, share, 1)
    solved = pl.pallas_call(
        lambda *refs: solve_lines(regions, *refs),
        out_shape=jax.ShapeDtypeStruct((features + 8, share), jnp.float32),
        scratch_shapes=[pltpu.VMEM((features, features, share), jnp.float32)],
        name="solve_lines",
    )(packed, weight_share, policy_share)
    steps, sums = gather_steps(solved, features)
    full_step = steps.transpose(1, 0, 2).reshape(features, lines_here)
    decrement_sq, norm_sq = jnp.sum(sums[:2], axis=1)

    total_lines = lines_here * ring
    step_length = 1.0 / (1.0 + jnp.sqrt(decrement_sq / (barrier_weight * features * total_lines)))
    new_policy = policy + step_length * full_step
    shift_flow = (
        lax.dot_general(factors, full_step, over_first, precision=HIGH)
        + full_step[regions][None, :] * ends_diff
    )
    new_flows = line_flow + step_length * shift_flow
    return (new_policy, new_flows, jnp.sqrt(decrement_sq), jnp.sqrt(norm_sq))


def solution(mesh):
    placed = (
        P("sample", "line"),
        P("line", None),
        P(),
        P(),
        P("line"),
        P(),
        P("line"),
        P("line"),
        P(None, "line"),
    )
    return jax.shard_map(
        shards,
        mesh=mesh,
        in_specs=placed,
        out_specs=(P(None, "line"), P("sample", "line"), P(), P()),
        check_vma=False,
    )
```
